32 devices in a mesh: dp: 1 (over z), sw: 4 (over y), sh: 8 (over x, core).
Axes of the slice: x: 4, y: 4, z: 1, core: 2. Of those that a mesh axis runs over, the one named last changes fastest.
The devices are a block of a 4x4x8 slice.
Arguments:
- features: bfloat16 [1, 768, 3, 64, 32], P('dp', None, None, 'sh', 'sw')
- latent: bfloat16 [1, 12, 3, 64, 32], P('dp', None, None, 'sh', 'sw')
- gn_gain: float32 [2, 2, 768], replicated
- gn_bias: float32 [2, 2, 768], replicated
- zy_weight: bfloat16 [2, 2, 12, 768], replicated
- zy_bias: float32 [2, 2, 768], replicated
- zb_weight: bfloat16 [2, 2, 12, 768], replicated
- zb_bias: float32 [2, 2, 768], replicated
- conv_weight: bfloat16 [2, 2, 768, 768, 3, 3, 3], replicated
- conv_bias: float32 [2, 2, 768], replicated
- up_weight: bfloat16 [768, 768, 3, 3], replicated
- up_bias: float32 [768], replicated
Outputs:
- output: bfloat16 [1, 768, 3, 128, 64], P('dp', None, None, 'sh', 'sw')
All inputs are finite; a program needn't handle non-finite values.
Results may differ from the reference program's by a relative error of at most 0.0125931.
Values are sent between devices in bfloat16 or wider.
A program may use at most 768 MiB of HBM per device.

```python
import jax
import jax.numpy as jnp
from jax import lax

CHANNELS = 768
LATENT = 12
GROUPS = 32
RES_BLOCKS = 2
FRAMES = 3
HEIGHT = 64
WIDTH = 32
GN_EPSILON = 1e-6
CONV_DIMS = ("NCDHW", "OIDHW", "NCDHW")


def setup_inputs(seed: int = 0, part: int = 0) -> dict:
    part_key = jax.random.fold_in(jax.random.key(seed), part)
    data_keys = jax.random.split(part_key, 6)
    weight_keys = jax.random.split(jax.random.key(seed + 1), 10)
    ramp_h = jnp.linspace(-1.0, 1.0, HEIGHT)[:, None]
    ramp_w = jnp.linspace(-1.0, 1.0, WIDTH)[None, :]
    amp_rows = jax.random.normal(data_keys[0], (CHANNELS, 1, 1, 1), jnp.float32)
    amp_cols = jax.random.normal(data_keys[1], (CHANNELS, 1, 1, 1), jnp.float32)
    noise = jax.random.normal(data_keys[2], (CHANNELS, FRAMES, HEIGHT, WIDTH), jnp.float32)
    features = (noise + amp_rows * ramp_h + amp_cols * ramp_w)[None].astype(jnp.bfloat16)
    lat_rows = jax.random.normal(data_keys[3], (LATENT, 1, 1, 1), jnp.float32)
    lat_cols = jax.random.normal(data_keys[4], (LATENT, 1, 1, 1), jnp.float32)
    lat_noise = jax.random.normal(data_keys[5], (LATENT, FRAMES, HEIGHT, WIDTH), jnp.float32)
    latent = (lat_noise + lat_rows * ramp_h + lat_cols * ramp_w)[None].astype(jnp.bfloat16)
    vec_shape = (RES_BLOCKS, 2, CHANNELS)
    map_shape = (RES_BLOCKS, 2, LATENT, CHANNELS)
    gn_gain = 1.0 + 0.3 * jax.random.normal(weight_keys[0], vec_shape, jnp.float32)
    gn_bias = 0.3 * jax.random.normal(weight_keys[1], vec_shape, jnp.float32)
    zy_weight = (jax.random.normal(weight_keys[2], map_shape, jnp.float32) * (0.5 * LATENT ** -0.5)).astype(jnp.bfloat16)
    zy_bias = 1.0 + 0.3 * jax.random.normal(weight_keys[3], vec_shape, jnp.float32)
    zb_weight = (jax.random.normal(weight_keys[4], map_shape, jnp.float32) * (0.5 * LATENT ** -0.5)).astype(jnp.bfloat16)
    zb_bias = 0.3 * jax.random.normal(weight_keys[5], vec_shape, jnp.float32)
    conv_weight = (jax.random.normal(weight_keys[6], (RES_BLOCKS, 2, CHANNELS, CHANNELS, 3, 3, 3), jnp.float32) * (27 * CHANNELS) ** -0.5).astype(jnp.bfloat16)
    conv_bias = 0.3 * jax.random.normal(weight_keys[7], vec_shape, jnp.float32)
    up_weight = (jax.random.normal(weight_keys[8], (CHANNELS, CHANNELS, 3, 3), jnp.float32) * (9 * CHANNELS) ** -0.5).astype(jnp.bfloat16)
    up_bias = 0.3 * jax.random.normal(weight_keys[9], (CHANNELS,), jnp.float32)
    return {"features": features, "latent": latent, "gn_gain": gn_gain, "gn_bias": gn_bias, "zy_weight": zy_weight, "zy_bias": zy_bias, "zb_weight": zb_weight, "zb_bias": zb_bias, "conv_weight": conv_weight, "conv_bias": conv_bias, "up_weight": up_weight, "up_bias": up_bias}


def per_channel(values):
    return values[None, :, None, None, None]


def group_norm(values, gain, shift):
    grouped = values.astype(jnp.float32).reshape(1, GROUPS, CHANNELS // GROUPS, FRAMES, HEIGHT, WIDTH)
    group_mean = jnp.mean(grouped, axis=(2, 3, 4, 5), keepdims=True)
    group_var = jnp.mean(jnp.square(grouped - group_mean), axis=(2, 3, 4, 5), keepdims=True)
    normed = ((grouped - group_mean) * lax.rsqrt(group_var + GN_EPSILON)).reshape(1, CHANNELS, FRAMES, HEIGHT, WIDTH)
    return normed * per_channel(gain) + per_channel(shift)


def latent_map(latent, weight, bias):
    return jnp.einsum("nzthw,zc->ncthw", latent.astype(jnp.float32), weight.astype(jnp.float32)) + per_channel(bias)


def causal_conv(activated, weight, bias):
    first_frame = activated[:, :, :1]
    padded = jnp.concatenate([first_frame, first_frame, activated], axis=2)
    padded = jnp.pad(padded, ((0, 0), (0, 0), (0, 0), (1, 1), (1, 1)))
    conv_out = lax.conv_general_dilated(padded.astype(jnp.float32), weight.astype(jnp.float32), (1, 1, 1), "VALID", dimension_numbers=CONV_DIMS)
    return (conv_out + per_channel(bias)).astype(jnp.bfloat16)


def reference(features, latent, gn_gain, gn_bias, zy_weight, zy_bias, zb_weight, zb_bias, conv_weight, conv_bias, up_weight, up_bias):
    hidden = features
    for block in range(RES_BLOCKS):
        branch = hidden
        for slot in range(2):
            normed = group_norm(branch, gn_gain[block, slot], gn_bias[block, slot])
            mixed = normed * latent_map(latent, zy_weight[block, slot], zy_bias[block, slot]) + latent_map(latent, zb_weight[block, slot], zb_bias[block, slot])
            activated = jax.nn.silu(mixed).astype(jnp.bfloat16)
            branch = causal_conv(activated, conv_weight[block, slot], conv_bias[block, slot])
        hidden = (hidden.astype(jnp.float32) + branch.astype(jnp.float32)).astype(jnp.bfloat16)
    upsampled = jnp.repeat(jnp.repeat(hidden, 2, axis=3), 2, axis=4)
    padded = jnp.pad(upsampled, ((0, 0), (0, 0), (0, 0), (1, 1), (1, 1)))
    conv_out = lax.conv_general_dilated(padded.astype(jnp.float32), up_weight[:, :, None].astype(jnp.float32), (1, 1, 1), "VALID", dimension_numbers=CONV_DIMS)
    return (conv_out + per_channel(up_bias)).astype(jnp.bfloat16)
```

```python
import functools

import jax
import jax.numpy as jnp
from jax import lax
from jax.experimental import pallas as pl
from jax.experimental.pallas import tpu as pltpu
from jax.sharding import PartitionSpec as P

NUM_GROUPS = 32
GN_EPSILON = 1e-6
TILE = 256
LANES = 128
SUB = 8
SLOTS = 12
EXPLICIT = False
F32 = jnp.float32
BF16 = jnp.bfloat16
MESH = pl.DeviceIdType.MESH
VMEM_BYTES = 66 * 1000 * 1000
SIDES = ((0, (1, 0)), (1, (-1, 0)), (2, (0, 1)), (3, (0, -1)))
CORNERS = ((0, (1, 1)), (1, (1, -1)), (2, (-1, 1)), (3, (-1, -1)))


class Mxu:
    def __init__(self):
        self.count = [0, 0]
        self.staged = None

    def push(self, rhs, q, transpose=False, value_transpose=False):
        reg = self.count[q] % 2
        self.count[q] += 1
        if EXPLICIT:
            if transpose and value_transpose:
                pltpu.matmul_push_rhs(rhs.T, staging_register=reg, mxu_index=q)
            else:
                pltpu.matmul_push_rhs(rhs, staging_register=reg, mxu_index=q, transpose=transpose)
        else:
            self.staged = rhs.T if transpose else rhs
        return reg

    def acc(self, ref, lhs, reg):
        if EXPLICIT:
            pltpu.matmul_acc_lhs(ref, lhs, load_staged_rhs=reg)
        else:
            ref[...] += jnp.dot(lhs.astype(BF16), self.staged, preferred_element_type=F32)

    def more(self, ref, lhs):
        if EXPLICIT:
            pltpu.matmul_acc_lhs(ref, lhs)
        else:
            ref[...] += jnp.dot(lhs.astype(BF16), self.staged, preferred_element_type=F32)

    def pop(self, ref):
        if EXPLICIT:
            return pltpu.matmul_pop(ref)
        val = ref[...]
        ref[...] = jnp.zeros_like(val)
        return val


def acc_ref(q, rows):
    return pltpu.ACC(q)((rows, TILE), F32) if EXPLICIT else pltpu.VMEM((rows, TILE), F32)


def split3(v):
    hi = v.astype(BF16)
    rest = v - hi.astype(F32)
    mid = rest.astype(BF16)
    low = (rest - mid.astype(F32)).astype(BF16)
    return hi, mid, low


def rounded(v):
    return v.astype(BF16).astype(F32)


def kernel(n_sh, n_sw, dims, feat, lat, gain, shift, zyb, zbb, cb, zyw, zbw, upb, wconv, wup, out,
           ring, xs, rf, xf, hact, zy, zb, zf, zw, par, gm, sums, msg, peers, side_out, corner_out, side_in, corner_in,
           tsum, yout, ring_sem, stat_send, stat_recv, halo_send, halo_recv):
    n_chan, n_frame, n_row, n_col, n_lat = dims
    n_pos = n_row * n_col
    n_tile = n_chan // TILE
    n_dev = n_sh * n_sw
    n_conv = 4
    n_tap = 9
    zlane = n_chan
    wide = n_chan + LANES
    sh = lax.axis_index("sh")
    sw = lax.axis_index("sw")
    me = sw * n_sh + sh
    count = float((n_chan // NUM_GROUPS) * n_frame * n_pos * n_dev)
    mxu = Mxu()
    total = n_conv * n_tap + 3

    def conv_copy(conv, tap, kt, slot):
        return pltpu.make_async_copy(wconv.at[conv, kt, tap], ring.at[slot, kt], ring_sem.at[slot])

    def up_copy(kh, kw, slot):
        return pltpu.make_async_copy(wup.at[kh * 3 + kw], ring.at[slot, kw], ring_sem.at[slot])

    def wait_chunk(slot):
        pltpu.make_async_copy(wconv.at[0, pl.ds(0, 3), 0], ring.at[slot], ring_sem.at[slot]).wait()

    def refill(g):
        nxt = g + SLOTS
        slot = lax.rem(g, SLOTS)

        @pl.when(nxt < n_conv * n_tap)
        def _():
            conv = nxt // n_tap
            for kt in range(3):
                conv_copy(conv, nxt - conv * n_tap, kt, slot).start()

        @pl.when((nxt >= n_conv * n_tap) & (nxt < total))
        def _():
            for kw in range(3):
                up_copy(nxt - n_conv * n_tap, kw, slot).start()

    for g in range(SLOTS):
        for kt in range(3):
            conv_copy(g // n_tap, g % n_tap, kt, g).start()
    side_in[...] = jnp.zeros_like(side_in)
    corner_in[...] = jnp.zeros_like(corner_in)

    def peer(step):
        dev = lax.rem(me + step, n_dev)
        return {"sw": dev // n_sh, "sh": lax.rem(dev, n_sh)}

    barrier = pltpu.get_barrier_semaphore()

    def tell(step, carry):
        pl.semaphore_signal(barrier, inc=1, device_id=peer(step), device_id_type=MESH)
        return carry

    lax.fori_loop(1, n_dev, tell, 0)

    for b in range(2):
        for s in range(2):
            for row, ref in enumerate((gain, shift, zyb, zbb, cb)):
                par[2 * b + s, row:row + 1, :] = ref[b, s:s + 1, :]
    zw[...] = jnp.zeros_like(zw)
    for which, ref in enumerate((zyw, zbw)):
        for b in range(2):
            for k in range(n_lat):
                pair = ref[b, k].astype(F32)
                for s in range(2):
                    zw[2 * b + s, which, k:k + 1, :] = pair[s:s + 1, :]
    zf[...] = jnp.zeros_like(zf)
    zf[0:n_frame * n_pos, 0:n_lat] = lat[...].astype(F32)
    chan_iota = lax.broadcasted_iota(jnp.int32, (TILE, TILE), 0)
    group_iota = lax.broadcasted_iota(jnp.int32, (TILE, TILE), 1) * (n_chan // NUM_GROUPS)
    for n in range(n_tile):
        off = chan_iota + n * TILE - group_iota
        gm[n] = jnp.where((off >= 0) & (off < n_chan // NUM_GROUPS), 1.0, 0.0).astype(BF16)
    start = feat[...].astype(F32)
    rf[...] = start
    xf[...] = start
    sums[0:SUB, :] = jnp.sum(start.reshape(-1, SUB, n_chan), axis=0)
    sums[SUB:, :] = jnp.sum(jnp.square(start).reshape(-1, SUB, n_chan), axis=0)
    sub_iota = lax.broadcasted_iota(jnp.int32, (SUB, n_chan), 0)

    def gather_rows(ref, at, step, n, cols):
        lanes = cols.stop - cols.start
        iota = lax.broadcasted_iota(jnp.int32, (SUB, lanes), 0)
        piece = jnp.zeros((SUB, lanes), F32)
        for i in range(n):
            row = jnp.broadcast_to(ref[at + i * step:at + i * step + 1, cols], (SUB, lanes))
            piece = jnp.where(iota == i, row, piece)
        return piece.astype(BF16)

    def stage(ref, lane0, lanes):
        cols = slice(0, lanes)
        put = slice(lane0, lane0 + lanes)
        for t in range(n_frame):
            base = t * n_pos
            side_out[0, t, :, put] = ref[base + n_pos - n_col:base + n_pos, cols].astype(BF16)
            side_out[1, t, :, put] = ref[base:base + n_col, cols].astype(BF16)
            side_out[2, t, :, put] = gather_rows(ref, base + n_col - 1, n_col, n_row, cols)
            side_out[3, t, :, put] = gather_rows(ref, base, n_col, n_row, cols)
        for d, at in enumerate((n_pos - 1, n_pos - n_col, n_col - 1, 0)):
            corner_out[d, :, put] = gather_rows(ref, at, n_pos, n_frame, cols)

    stage(zf, zlane, LANES)

    def inside(row, col):
        ok = None
        for step, pos, n in ((row, sh, n_sh), (col, sw, n_sw)):
            if step == 0:
                continue
            one = pos + step < n if step > 0 else pos + step >= 0
            ok = one if ok is None else ok & one
        return ok

    def halo_copies(slot):
        found = []
        for kind, (outs, ins, steps) in enumerate(((side_out, side_in, SIDES), (corner_out, corner_in, CORNERS))):
            for d, (row, col) in steps:
                copy = pltpu.make_async_remote_copy(
                    src_ref=outs.at[d], dst_ref=ins.at[slot, d], send_sem=halo_send.at[kind * 4 + d],
                    recv_sem=halo_recv.at[slot, kind * 4 + d], device_id={"sh": sh + row, "sw": sw + col}, device_id_type=MESH)
                found.append((copy, inside(row, col), inside(-row, -col)))
        return found

    def halo_start(slot):
        for copy, to, _ in halo_copies(slot):
            @pl.when(to)
            def _():
                copy.start()

    def halo_wait(slot):
        for copy, to, source in halo_copies(slot):
            @pl.when(source)
            def _():
                copy.wait_recv()

            @pl.when(to)
            def _():
                copy.wait_send()

    def stat_copy(slot, step):
        return pltpu.make_async_remote_copy(
            src_ref=msg, dst_ref=peers.at[slot, me], send_sem=stat_send, recv_sem=stat_recv.at[slot],
            device_id=peer(step), device_id_type=MESH)

    def stat_all(slot):
        part = peers.at[slot, pl.ds(0, n_dev - 1)]
        return pltpu.make_async_remote_copy(
            src_ref=part, dst_ref=part, send_sem=stat_send, recv_sem=stat_recv.at[slot], device_id=peer(1), device_id_type=MESH)

    def stats_start(slot, aux):
        for k in range(n_tile):
            reg = mxu.push(gm[k], 0)
            for i, piece in enumerate(split3(sums[:, k * TILE:(k + 1) * TILE])):
                if i == 0:
                    mxu.acc(aux, piece, reg)
                else:
                    mxu.more(aux, piece)
        got = mxu.pop(aux)[:, 0:LANES]
        mine = jnp.concatenate([jnp.sum(got[0:SUB], axis=0, keepdims=True), jnp.sum(got[SUB:], axis=0, keepdims=True)], axis=0)
        msg[...] = mine
        peers[slot, me] = mine

        def go(step, carry):
            stat_copy(slot, step).start()
            return carry

        lax.fori_loop(1, n_dev, go, 0)

    def stats_finish(slot, aux):
        both = stat_all(slot)
        both.wait_recv()
        both.wait_send()
        tot = jnp.sum(peers[slot], axis=0)
        mean = tot[0:1] / count
        var = jnp.maximum(tot[1:2] / count - jnp.square(mean), 0.0)
        inv = lax.rsqrt(var + GN_EPSILON)
        rows = lax.broadcasted_iota(jnp.int32, (2 * SUB, LANES), 0)
        left = jnp.where(rows == 0, mean, jnp.where(rows == 1, inv, 0.0))
        lhs = jnp.concatenate([left, jnp.zeros_like(left)], axis=1)
        pieces = split3(lhs)
        found = []
        for n in range(n_tile):
            reg = mxu.push(gm[n], n % 2, transpose=True)
            for i, piece in enumerate(pieces):
                if i == 0:
                    mxu.acc(aux[n], piece, reg)
                else:
                    mxu.more(aux[n], piece)
        for n in range(n_tile):
            found.append(mxu.pop(aux[n]))
        whole = jnp.concatenate(found, axis=1)
        return whole[0:1], whole[1:2]

    def latent_maps(conv, accs):
        n_own = n_frame * n_pos
        zeros = jnp.zeros((TILE - 2 * SUB, TILE), BF16)
        for which, (dst, row) in enumerate(((zy, 2), (zb, 3))):
            for n in range(n_tile):
                q = n % 2
                cols = slice(n * TILE, (n + 1) * TILE)
                w = jnp.concatenate([zw[conv, which, :, cols].astype(BF16), zeros], axis=0)
                bias = par[conv, row:row + 1, cols]
                reg = mxu.push(w, q)
                mxu.acc(accs[q][0][2], zf[0:n_own, :], reg)
                mxu.more(accs[q][0][1], zf[n_own:, :])
                dst[0:n_own, cols] = mxu.pop(accs[q][0][2]) + bias
                dst[n_own:, cols] = mxu.pop(accs[q][0][1]) + bias

    halo_flags = [inside(-row, -col) for _, (row, col) in SIDES] + [inside(-row, -col) for _, (row, col) in CORNERS]

    def halo_values(slot, q):
        if q < 4 * n_frame:
            return side_in[slot, q // n_frame, q % n_frame, :, 0:n_chan].astype(F32), halo_flags[q // n_frame]
        return corner_in[slot, q - 4 * n_frame, :, 0:n_chan].astype(F32), halo_flags[4 + q - 4 * n_frame]

    n_side = n_frame * SUB

    def put_rows(t, at, mid, before, after):
        xs[1, t, pl.ds(at, SUB), :] = mid
        xs[0, t, pl.ds(at, SUB), :] = jnp.where(sub_iota == 0, before, pltpu.roll(mid, 1, axis=0))
        xs[2, t, pl.ds(at, SUB), :] = jnp.where(sub_iota == SUB - 1, after, pltpu.roll(mid, SUB - 1, axis=0))

    def build(slot, value_fn):
        for q in range(4 * n_frame + 4):
            v, flag = halo_values(slot, q)
            hact[q * SUB:(q + 1) * SUB, :] = jnp.where(flag, value_fn(v, n_frame * n_pos + q * SUB), 0.0)
        for t in range(n_frame):
            for at, side, corner in ((0, 0, 0), ((n_row + 1) * SUB, 1, 2)):
                mid = hact[side * n_side + t * SUB:side * n_side + (t + 1) * SUB, :]
                c0 = 4 * n_side + corner * SUB + t
                put_rows(t, at, mid, hact[c0:c0 + 1, :], hact[c0 + SUB:c0 + SUB + 1, :])

        def rows(g, carry):
            at = pl.multiple_of(g * SUB, SUB)
            t = g // n_row
            mid = value_fn(rf[pl.ds(at, SUB), :], at)
            put_rows(t, pl.multiple_of((g - t * n_row + 1) * SUB, SUB), mid, hact[pl.ds(2 * n_side + g, 1), :], hact[pl.ds(3 * n_side + g, 1), :])
            return carry

        lax.fori_loop(0, n_frame * n_row, rows, 0, unroll=4)

    def convs(*accs_flat):
        aux = accs_flat[:3]
        conv_acc = accs_flat[15:]
        accs_flat = accs_flat[:15]
        accs = [[dict(zip((0, 1, 2), accs_flat[3 + 6 * q + 3 * i:6 + 6 * q + 3 * i])) for i in range(2)] for q in range(2)]
        for ref in accs_flat:
            mxu.pop(ref)
        pl.semaphore_wait(barrier, n_dev - 1)

        def one_conv(conv, carry):
            slot = lax.rem(conv, 2)
            stats_start(slot, aux[0])
            stage(rf, 0, n_chan)
            halo_start(slot)
            halo_wait(slot)

            @pl.when(conv == 0)
            def _():
                n_own = n_frame * n_pos
                for q in range(4 * n_frame):
                    zf[n_own + q * SUB:n_own + (q + 1) * SUB, 0:LANES] = side_in[slot, q // n_frame, q % n_frame, :, zlane:wide].astype(F32)
                for q in range(4):
                    at = n_own + (4 * n_frame + q) * SUB
                    zf[at:at + SUB, 0:LANES] = corner_in[slot, q, :, zlane:wide].astype(F32)

            latent_maps(conv, accs)
            mean, inv = stats_finish(slot, aux)
            scale = inv * par[conv, 0:1, :]
            offset = par[conv, 1:2, :]

            def act(v, at):
                normed = (v - mean) * scale + offset
                mixed = normed * zy[pl.ds(at, SUB), :] + zb[pl.ds(at, SUB), :]
                return rounded(mixed / (1.0 + jnp.exp(-mixed)))

            build(slot, act)

            def tap(p, carry):
                g = conv * n_tap + p
                ring_slot = lax.rem(g, SLOTS)
                kh = p // 3
                kw = p - 3 * kh
                wait_chunk(ring_slot)
                at = pl.multiple_of(kh * SUB, SUB)
                for kt in (2, 1, 0):
                    lhs = xs[kw, 0:kt + 1, pl.ds(at, n_pos), :].reshape((kt + 1) * n_pos, n_chan).astype(BF16)
                    conv_acc[kt][...] += lax.dot_general(lhs, ring[ring_slot, kt], (((1,), (1,)), ((), ())), preferred_element_type=F32)
                refill(g)
                return carry

            for ref in conv_acc:
                ref[...] = jnp.zeros_like(ref)
            lax.fori_loop(0, n_tap, tap, 0)

            odd = lax.rem(conv, 2) == 1
            for n in range(n_tile):
                cols = slice(n * TILE, (n + 1) * TILE)
                r2, r1, r0 = [conv_acc[kt][:, cols] for kt in (2, 1, 0)]
                bias = par[conv, 4:5, cols]
                s1 = jnp.zeros((SUB, TILE), F32)
                s2 = jnp.zeros((SUB, TILE), F32)
                for t in range(n_frame):
                    early = max(t - 1, 0)
                    rows = slice(t * n_pos, (t + 1) * n_pos)
                    y = rounded(r2[rows] + r1[early * n_pos:(early + 1) * n_pos] + r0 + bias)
                    old = xf[rows, cols]
                    x = jnp.where(odd, rounded(old + y), y)
                    xf[rows, cols] = jnp.where(odd, x, old)
                    rf[rows, cols] = x
                    s1 += jnp.sum(x.reshape(-1, SUB, TILE), axis=0)
                    s2 += jnp.sum(jnp.square(x).reshape(-1, SUB, TILE), axis=0)
                sums[0:SUB, cols] = s1
                sums[SUB:, cols] = s2
            return carry

        lax.fori_loop(0, n_conv, one_conv, 0)

    specs = [acc_ref(0, 2 * SUB), acc_ref(1, 2 * SUB), acc_ref(0, 2 * SUB)]
    for q in range(2):
        for _ in range(2):
            specs += [acc_ref(q, (kt + 1) * n_pos) for kt in range(3)]
    specs += [pltpu.VMEM(((kt + 1) * n_pos, n_chan), F32) for kt in range(3)]
    pl.run_scoped(convs, *specs)

    stage(rf, 0, n_chan)
    last = n_conv % 2
    halo_start(last)
    halo_wait(last)
    build(last, lambda v, at: v)
    n_up = (n_row + 1) * n_col

    def upsample(*accs_flat):
        accs = [accs_flat[3 * q:3 * q + 3] for q in range(2)]
        for ref in accs_flat:
            mxu.pop(ref)
        for kh in range(3):
            g = n_conv * n_tap + kh
            ring_slot = g % SLOTS
            wait_chunk(ring_slot)
            at = SUB * min(kh, 1)
            for n in range(n_tile):
                q = (kh * n_tile + n) % 2
                cols = slice(n * TILE, (n + 1) * TILE)
                for kw, uses in ((0, ((0, 0), (1, 2))), (2, ((1, 0), (2, 2))), (1, ((1, 1),))):
                    for k in range(n_tile):
                        ks = slice(k * TILE, (k + 1) * TILE)
                        reg = mxu.push(ring[ring_slot, kw, cols, ks], q, transpose=True)
                        for i, (shifted, group) in enumerate(uses):
                            lhs = xs[shifted, :, at:at + n_up, ks].reshape(n_frame * n_up, TILE)
                            if i == 0:
                                mxu.acc(accs[q][group], lhs, reg)
                            else:
                                mxu.more(accs[q][group], lhs)
                first, last_, both = mxu.pop(accs[q][0]), mxu.pop(accs[q][2]), mxu.pop(accs[q][1])
                tsum[kh, 0, :, cols] = first + both
                tsum[kh, 1, :, cols] = last_ + both

    pl.run_scoped(upsample, *[acc_ref(q, n_frame * n_up) for q in range(2) for _ in range(3)])

    bias = upb[...]
    n_up_rows = n_row + 1

    def finish(g, carry):
        t = g // n_row
        i = g - t * n_row
        here = t * n_up + i * SUB
        for a in range(2):
            for b in range(2):
                v = bias
                for kh in range(3):
                    down = SUB if (a == 1 and kh != 1) else 0
                    v = v + tsum[kh, b, pl.ds(pl.multiple_of(here + down, SUB), SUB), :]
                for j in range(n_chan // LANES):
                    yout[a, j, pl.ds(b, SUB, stride=2), :] = v[:, j * LANES:(j + 1) * LANES]
            for j in range(n_chan // LANES):
                out[t, 2 * i + a, :, j * LANES:(j + 1) * LANES] = yout[a, j].astype(BF16)
        return carry

    lax.fori_loop(0, n_frame * n_row, finish, 0)


XLU_TILES = ()


def solution(mesh):
    n_sh = mesh.shape["sh"]
    n_sw = mesh.shape["sw"]
    n_dev = n_sh * n_sw

    def local_step(features, latent, gn_gain, gn_bias, zy_weight, zy_bias, zb_weight, zb_bias, conv_weight, conv_bias, up_weight, up_bias):
        _, n_chan, n_frame, n_row, n_col = features.shape
        n_lat = latent.shape[1]
        n_pos = n_row * n_col
        n_own = n_frame * n_pos
        n_halo = (4 * n_frame + 4) * SUB
        feat = jnp.transpose(features, (0, 2, 3, 4, 1)).reshape(n_own, n_chan)
        lat = jnp.transpose(latent, (0, 2, 3, 4, 1)).reshape(n_own, n_lat)
        wconv = jnp.transpose(conv_weight, (0, 1, 4, 5, 6, 2, 3)).reshape(4, 3, 9, n_chan, n_chan)
        wup = jnp.transpose(up_weight, (2, 3, 0, 1)).reshape(9, n_chan, n_chan)
        zyw = jnp.transpose(zy_weight, (0, 2, 1, 3))
        zbw = jnp.transpose(zb_weight, (0, 2, 1, 3))
        vmem = pl.BlockSpec(memory_space=pltpu.VMEM)
        hbm = pl.BlockSpec(memory_space=pl.ANY)
        wide = n_chan + LANES
        y = pl.pallas_call(
            functools.partial(kernel, n_sh, n_sw, (n_chan, n_frame, n_row, n_col, n_lat)),
            out_shape=jax.ShapeDtypeStruct((n_frame, 2 * n_row, 2 * n_col, n_chan), BF16),
            in_specs=[vmem] * 10 + [hbm] * 2,
            out_specs=vmem,
            scratch_shapes=[
                pltpu.VMEM((SLOTS, 3, n_chan, n_chan), BF16),
                pltpu.VMEM((3, n_frame, (n_row + 2) * SUB, n_chan), F32),
                pltpu.VMEM((n_own, n_chan), F32),
                pltpu.VMEM((n_own, n_chan), F32),
                pltpu.VMEM((n_halo, n_chan), F32),
                pltpu.VMEM((n_own + n_halo, n_chan), F32),
                pltpu.VMEM((n_own + n_halo, n_chan), F32),
                pltpu.VMEM((n_own + n_halo, TILE), F32),
                pltpu.VMEM((4, 2, 2 * SUB, n_chan), F32),
                pltpu.VMEM((4, SUB, n_chan), F32),
                pltpu.VMEM((n_chan // TILE, TILE, TILE), BF16),
                pltpu.VMEM((2 * SUB, n_chan), F32),
                pltpu.VMEM((2, LANES), F32),
                pltpu.VMEM((2, n_dev, 2, LANES), F32),
                pltpu.VMEM((4, n_frame, SUB, wide), BF16),
                pltpu.VMEM((4, SUB, wide), BF16),
                pltpu.VMEM((2, 4, n_frame, SUB, wide), BF16),
                pltpu.VMEM((2, 4, SUB, wide), BF16),
                pltpu.VMEM((3, 2, n_frame * (n_row + 1) * n_col, n_chan), F32),
                pltpu.VMEM((2, n_chan // LANES, 2 * n_col, LANES), F32),
                pltpu.SemaphoreType.DMA((SLOTS,)),
                pltpu.SemaphoreType.DMA,
                pltpu.SemaphoreType.DMA((2,)),
                pltpu.SemaphoreType.DMA((8,)),
                pltpu.SemaphoreType.DMA((2, 8)),
            ],
            compiler_params=pltpu.CompilerParams(collective_id=0, has_side_effects=True, vmem_limit_bytes=VMEM_BYTES),
        )(feat, lat, gn_gain, gn_bias, zy_bias, zb_bias, conv_bias, zyw, zbw, up_bias.reshape(1, n_chan), wconv, wup)
        return jnp.transpose(y.reshape(1, n_frame, 2 * n_row, 2 * n_col, n_chan), (0, 4, 1, 2, 3))

    data_spec = P("dp", None, None, "sh", "sw")
    return jax.shard_map(local_step, mesh=mesh, in_specs=(data_spec, data_spec) + (P(),) * 10, out_specs=data_spec, check_vma=False)
```

```python
import functools

import jax
import jax.numpy as jnp
from jax import lax
from jax.experimental import pallas as pl
from jax.experimental.pallas import tpu as pltpu
from jax.sharding import PartitionSpec as P

NUM_GROUPS = 32
GN_EPSILON = 1e-6
TILE = 256
LANES = 128
SUB = 8
SLOTS = 12
GROUP = 3
F32 = jnp.float32
BF16 = jnp.bfloat16
MESH = pl.DeviceIdType.MESH
VMEM_BYTES = 66 * 1000 * 1000
SIDES = ((0, (1, 0)), (1, (-1, 0)), (2, (0, 1)), (3, (0, -1)))
CORNERS = ((0, (1, 1)), (1, (1, -1)), (2, (-1, 1)), (3, (-1, -1)))


def split3(v):
    hi = v.astype(BF16)
    rest = v - hi.astype(F32)
    mid = rest.astype(BF16)
    low = (rest - mid.astype(F32)).astype(BF16)
    return hi, mid, low


def rounded(v):
    return v.astype(BF16).astype(F32)


def dot(a, b):
    return jnp.dot(a, b, preferred_element_type=F32)


def dot_nt(a, b):
    return lax.dot_general(a, b, (((1,), (1,)), ((), ())), preferred_element_type=F32)


def peer_steps(n_sh, n_sw):
    cores = 2 if n_sh % 2 == 0 else 1
    n_x = n_sh // cores
    steps = [(x, y, c) for x in range(n_x) for y in range(n_sw) for c in range(cores)][1:]
    return cores, n_x, sorted(steps, key=lambda s: -(min(s[0], n_x - s[0]) + min(s[1], n_sw - s[1])))


def kernel(n_sh, n_sw, dims, feat, lat, gain, shift, zyb, zbb, cb, zyw, zbw, upb, wconv, wup, out,
           ring, xs, rf, xf, hact, zy, zb, zf, zw, par, gm, gmt, sums, msg, peers, side_out, corner_out, side_in, corner_in,
           acc_0, acc_1, acc_2, tsum, yout, ring_sem, stat_send, stat_recv, halo_send, halo_recv):
    n_chan, n_frame, n_row, n_col, n_lat = dims
    n_pos = n_row * n_col
    n_own = n_frame * n_pos
    n_dev = n_sh * n_sw
    n_conv = 4
    n_tap = 9
    zlane = n_chan
    wide = n_chan + LANES
    sh = lax.axis_index("sh")
    sw = lax.axis_index("sw")
    me = sw * n_sh + sh
    per_group = n_chan // NUM_GROUPS
    count = float(per_group * n_own * n_dev)
    total = n_conv * n_tap + 3
    accs = (acc_0, acc_1, acc_2)

    def conv_copy(conv, tap, kt, slot):
        return pltpu.make_async_copy(wconv.at[conv, kt, tap], ring.at[slot, kt], ring_sem.at[slot])

    def up_copy(kh, kw, slot):
        return pltpu.make_async_copy(wup.at[kh * 3 + kw], ring.at[slot, kw], ring_sem.at[slot])

    def wait_chunk(slot):
        pltpu.make_async_copy(wconv.at[0, pl.ds(0, 3), 0], ring.at[slot], ring_sem.at[slot]).wait()

    def refill(g):
        nxt = g + SLOTS
        slot = lax.rem(g, SLOTS)

        @pl.when(nxt < n_conv * n_tap)
        def _():
            conv = nxt // n_tap
            for kt in range(3):
                conv_copy(conv, nxt - conv * n_tap, kt, slot).start()

        @pl.when((nxt >= n_conv * n_tap) & (nxt < total))
        def _():
            for kw in range(3):
                up_copy(nxt - n_conv * n_tap, kw, slot).start()

    cores, n_x, steps = peer_steps(n_sh, n_sw)
    chip = sh // cores
    core = sh - chip * cores

    def peer(step):
        return {"sh": lax.rem(chip + step[0], n_x) * cores + lax.rem(core + step[2], cores), "sw": lax.rem(sw + step[1], n_sw)}

    barrier = pltpu.get_barrier_semaphore()
    for step in steps:
        pl.semaphore_signal(barrier, inc=1, device_id=peer(step), device_id_type=MESH)
    for g in range(SLOTS):
        for kt in range(3):
            conv_copy(g // n_tap, g % n_tap, kt, g).start()

    def gather_rows(ref, at, step, n, cols):
        lanes = cols.stop - cols.start
        iota = lax.broadcasted_iota(jnp.int32, (SUB, lanes), 0)
        piece = jnp.zeros((SUB, lanes), F32)
        for i in range(n):
            row = jnp.broadcast_to(ref[at + i * step:at + i * step + 1, cols], (SUB, lanes))
            piece = jnp.where(iota == i, row, piece)
        return piece.astype(BF16)

    def stage(ref, lane0, lanes):
        cols = slice(0, lanes)
        put = slice(lane0, lane0 + lanes)
        for t in range(n_frame):
            base = t * n_pos
            side_out[0, t, :, put] = ref[base + n_pos - n_col:base + n_pos, cols].astype(BF16)
            side_out[1, t, :, put] = ref[base:base + n_col, cols].astype(BF16)
            side_out[2, t, :, put] = gather_rows(ref, base + n_col - 1, n_col, n_row, cols)
            side_out[3, t, :, put] = gather_rows(ref, base, n_col, n_row, cols)
        for d, at in enumerate((n_pos - 1, n_pos - n_col, n_col - 1, 0)):
            corner_out[d, :, put] = gather_rows(ref, at, n_pos, n_frame, cols)

    def inside(row, col):
        ok = None
        for step, pos, n in ((row, sh, n_sh), (col, sw, n_sw)):
            if step == 0:
                continue
            one = pos + step < n if step > 0 else pos + step >= 0
            ok = one if ok is None else ok & one
        return ok

    def halo_copies(slot):
        found = []
        for kind, (outs, ins, ways) in enumerate(((side_out, side_in, SIDES), (corner_out, corner_in, CORNERS))):
            for d, (row, col) in ways:
                copy = pltpu.make_async_remote_copy(
                    src_ref=outs.at[d], dst_ref=ins.at[slot, d], send_sem=halo_send.at[kind * 4 + d],
                    recv_sem=halo_recv.at[slot, kind * 4 + d], device_id={"sh": sh + row, "sw": sw + col}, device_id_type=MESH)
                found.append((copy, inside(row, col), inside(-row, -col)))
        return found

    def halo_start(slot):
        for copy, to, _ in halo_copies(slot):
            @pl.when(to)
            def _():
                copy.start()

    def halo_wait(slot):
        for copy, to, source in halo_copies(slot):
            @pl.when(source)
            def _():
                copy.wait_recv()

            @pl.when(to)
            def _():
                copy.wait_send()

    def stat_copy(slot, step):
        return pltpu.make_async_remote_copy(
            src_ref=msg, dst_ref=peers.at[slot, me], send_sem=stat_send, recv_sem=stat_recv.at[slot],
            device_id=peer(step), device_id_type=MESH)

    def stat_all(slot):
        part = peers.at[slot, pl.ds(0, n_dev - 1)]
        return pltpu.make_async_remote_copy(
            src_ref=part, dst_ref=part, send_sem=stat_send, recv_sem=stat_recv.at[slot], device_id=peer(steps[0]), device_id_type=MESH)

    def group_sums(slot, values):
        got = dot(jnp.concatenate(split3(values), axis=0), gm[...])
        rows = got[0:2 * SUB] + got[2 * SUB:4 * SUB] + got[4 * SUB:6 * SUB]
        mine = jnp.concatenate([jnp.sum(rows[0:SUB], axis=0, keepdims=True), jnp.sum(rows[SUB:], axis=0, keepdims=True)], axis=0)
        msg[...] = mine
        peers[slot, me] = mine

    def stats_send(slot):
        for step in steps:
            stat_copy(slot, step).start()

    def stats_finish(slot):
        both = stat_all(slot)
        both.wait_recv()
        both.wait_send()
        tot = jnp.sum(peers[slot], axis=0)
        mean = tot[0:1] / count
        var = jnp.maximum(tot[1:2] / count - jnp.square(mean), 0.0)
        inv = lax.rsqrt(var + GN_EPSILON)
        rows = lax.broadcasted_iota(jnp.int32, (SUB, LANES), 0)
        lhs = jnp.where(rows == 0, mean, jnp.where(rows == 1, inv, 0.0))
        got = dot(jnp.concatenate(split3(lhs), axis=0), gmt[...])
        whole = got[0:SUB] + got[SUB:2 * SUB] + got[2 * SUB:3 * SUB]
        return whole[0:1], whole[1:2]

    def latent_maps(conv):
        got = dot(zf[...].astype(BF16), zw[conv])
        zy[...] = got[:, 0:n_chan] + par[conv, 2:3, :]
        zb[...] = got[:, n_chan:] + par[conv, 3:4, :]

    halo_flags = [inside(-row, -col) for _, (row, col) in SIDES] + [inside(-row, -col) for _, (row, col) in CORNERS]

    def halo_values(slot, q):
        if q < 4 * n_frame:
            return side_in[slot, q // n_frame, q % n_frame, :, 0:n_chan].astype(F32), halo_flags[q // n_frame]
        return corner_in[slot, q - 4 * n_frame, :, 0:n_chan].astype(F32), halo_flags[4 + q - 4 * n_frame]

    n_side = n_frame * SUB
    sub_iota = lax.broadcasted_iota(jnp.int32, (SUB, n_chan), 0)

    def put_rows(t, at, mid, before, after):
        xs[1, t, pl.ds(at, SUB), :] = mid
        xs[0, t, pl.ds(at, SUB), :] = jnp.where(sub_iota == 0, before, pltpu.roll(mid, 1, axis=0))
        xs[2, t, pl.ds(at, SUB), :] = jnp.where(sub_iota == SUB - 1, after, pltpu.roll(mid, SUB - 1, axis=0))

    def build(slot, value_fn):
        for q in range(4 * n_frame + 4):
            v, flag = halo_values(slot, q)
            hact[q * SUB:(q + 1) * SUB, :] = jnp.where(flag, value_fn(v, n_own + q * SUB), 0.0)
        for t in range(n_frame):
            for at, side, corner in ((0, 0, 0), ((n_row + 1) * SUB, 1, 2)):
                mid = hact[side * n_side + t * SUB:side * n_side + (t + 1) * SUB, :]
                c0 = 4 * n_side + corner * SUB + t
                put_rows(t, at, mid, hact[c0:c0 + 1, :], hact[c0 + SUB:c0 + SUB + 1, :])

        def rows(g, carry):
            at = pl.multiple_of(g * SUB, SUB)
            t = g // n_row
            mid = value_fn(rf[pl.ds(at, SUB), :], at)
            put_rows(t, pl.multiple_of((g - t * n_row + 1) * SUB, SUB), mid, hact[pl.ds(2 * n_side + g, 1), :], hact[pl.ds(3 * n_side + g, 1), :])
            return carry

        lax.fori_loop(0, n_frame * n_row, rows, 0, unroll=4)

    for ref, g_dim, c_dim in ((gm, 1, 0), (gmt, 0, 1)):
        off = lax.broadcasted_iota(jnp.int32, ref.shape, c_dim) - lax.broadcasted_iota(jnp.int32, ref.shape, g_dim) * per_group
        ref[...] = jnp.where((off >= 0) & (off < per_group), 1.0, 0.0).astype(BF16)
    start = feat[...].astype(F32)
    rf[...] = start
    xf[...] = start
    group_sums(0, jnp.concatenate([jnp.sum(start.reshape(-1, SUB, n_chan), axis=0), jnp.sum(jnp.square(start).reshape(-1, SUB, n_chan), axis=0)], axis=0))
    pl.semaphore_wait(barrier, n_dev - 1)
    stats_send(0)
    zf[...] = jnp.zeros_like(zf)
    zf[0:n_own, 0:n_lat] = lat[...].astype(F32)
    stage(zf, zlane, LANES)
    stage(rf, 0, n_chan)
    halo_start(0)
    for b in range(2):
        for s in range(2):
            for row, ref in enumerate((gain, shift, zyb, zbb, cb)):
                par[2 * b + s, row:row + 1, :] = ref[b, s:s + 1, :]
    for which, ref in enumerate((zyw, zbw)):
        put = slice(which * n_chan, (which + 1) * n_chan)
        for b in range(2):
            rows_k = lax.broadcasted_iota(jnp.int32, (2 * SUB, n_chan), 0)
            w = [jnp.zeros((2 * SUB, n_chan), F32) for _ in range(2)]
            for k in range(n_lat):
                pair = ref[b, k].astype(F32)
                w = [jnp.where(rows_k == k, jnp.broadcast_to(pair[s:s + 1, :], rows_k.shape), w[s]) for s in range(2)]
            for s in range(2):
                zw[2 * b + s, 0:2 * SUB, put] = w[s].astype(BF16)
    zw[:, 2 * SUB:, :] = jnp.zeros((4, LANES - 2 * SUB, 2 * n_chan), BF16)

    def one_conv(conv, carry):
        slot = lax.rem(conv, 2)
        halo_wait(slot)

        @pl.when(conv == 0)
        def _():
            for q in range(4 * n_frame):
                zf[n_own + q * SUB:n_own + (q + 1) * SUB, :] = side_in[slot, q // n_frame, q % n_frame, :, zlane:wide].astype(F32)
            for q in range(4):
                at = n_own + (4 * n_frame + q) * SUB
                zf[at:at + SUB, :] = corner_in[slot, q, :, zlane:wide].astype(F32)

        latent_maps(conv)
        mean, inv = stats_finish(slot)
        scale = inv * par[conv, 0:1, :]
        offset = par[conv, 1:2, :]

        def act(v, at):
            normed = (v - mean) * scale + offset
            mixed = normed * zy[pl.ds(at, SUB), :] + zb[pl.ds(at, SUB), :]
            return rounded(mixed / (1.0 + jnp.exp(-mixed)))

        build(slot, act)

        def taps(step, carry):
            for i in range(GROUP):
                wait_chunk(lax.rem(conv * n_tap + step * GROUP + i, SLOTS))
            for kt in (2, 1, 0):
                lhs, rhs = [], []
                for i in range(GROUP):
                    p = step * GROUP + i
                    kh = p // 3
                    kw = p - 3 * kh
                    at = pl.multiple_of(kh * SUB, SUB)
                    lhs.append(xs[kw, 0:kt + 1, pl.ds(at, n_pos), :].reshape((kt + 1) * n_pos, n_chan).astype(BF16))
                    rhs.append(ring[lax.rem(conv * n_tap + p, SLOTS), kt])
                accs[kt][...] += dot_nt(jnp.concatenate(lhs, axis=1), jnp.concatenate(rhs, axis=1))
            for i in range(GROUP):
                refill(conv * n_tap + step * GROUP + i)
            return carry

        for ref in accs:
            ref[...] = jnp.zeros_like(ref)
        lax.fori_loop(0, n_tap // GROUP, taps, 0)

        odd = lax.rem(conv, 2) == 1
        s1 = jnp.zeros((SUB, n_chan), F32)
        s2 = jnp.zeros((SUB, n_chan), F32)
        bias = par[conv, 4:5, :]
        for at in range(0, n_pos, SUB):
            shared = acc_0[at:at + SUB, :] + bias
            for t in range(n_frame):
                early = max(t - 1, 0) * n_pos + at
                row = t * n_pos + at
                y = rounded(acc_2[row:row + SUB, :] + acc_1[early:early + SUB, :] + shared)
                old = xf[row:row + SUB, :]
                x = jnp.where(odd, rounded(old + y), y)
                xf[row:row + SUB, :] = jnp.where(odd, x, old)
                rf[row:row + SUB, :] = x
                s1 += x
                s2 += jnp.square(x)
        after = 1 - slot
        group_sums(after, jnp.concatenate([s1, s2], axis=0))

        @pl.when(conv < n_conv - 1)
        def _():
            stats_send(after)

        stage(rf, 0, n_chan)
        halo_start(after)
        return carry

    lax.fori_loop(0, n_conv, one_conv, 0)

    last = n_conv % 2
    halo_wait(last)
    build(last, lambda v, at: v)
    n_up = (n_row + 1) * n_col
    m_up = n_frame * n_up

    def up_row(kh, carry):
        ring_slot = lax.rem(n_conv * n_tap + kh, SLOTS)
        wait_chunk(ring_slot)
        at = pl.multiple_of(jnp.minimum(kh, 1) * SUB, SUB)
        x = [xs[d, :, pl.ds(at, n_up), :].reshape(m_up, n_chan).astype(BF16) for d in range(3)]
        for n in range(n_chan // TILE):
            cols = slice(n * TILE, (n + 1) * TILE)
            side_a = dot_nt(jnp.concatenate([x[0], x[1]], axis=0), ring[ring_slot, 0, cols, :])
            both = dot_nt(x[1], ring[ring_slot, 1, cols, :])
            side_b = dot_nt(jnp.concatenate([x[1], x[2]], axis=0), ring[ring_slot, 2, cols, :])
            tsum[kh, 0, :, cols] = side_a[0:m_up] + both + side_b[0:m_up]
            tsum[kh, 1, :, cols] = side_a[m_up:] + both + side_b[m_up:]
        return carry

    lax.fori_loop(0, 3, up_row, 0)
    bias_up = upb[...]

    def finish(g, carry):
        t = g // n_row
        i = g - t * n_row
        here = t * n_up + i * SUB
        for a in range(2):
            for b in range(2):
                v = bias_up
                for kh in range(3):
                    down = SUB if (a == 1 and kh != 1) else 0
                    v = v + tsum[kh, b, pl.ds(pl.multiple_of(here + down, SUB), SUB), :]
                for j in range(n_chan // LANES):
                    yout[a, j, pl.ds(b, SUB, stride=2), :] = v[:, j * LANES:(j + 1) * LANES]
            for j in range(n_chan // LANES):
                out[t, 2 * i + a, :, j * LANES:(j + 1) * LANES] = yout[a, j].astype(BF16)
        return carry

    lax.fori_loop(0, n_frame * n_row, finish, 0)


def solution(mesh):
    n_sh = mesh.shape["sh"]
    n_sw = mesh.shape["sw"]
    n_dev = n_sh * n_sw

    def local_step(features, latent, gn_gain, gn_bias, zy_weight, zy_bias, zb_weight, zb_bias, conv_weight, conv_bias, up_weight, up_bias):
        _, n_chan, n_frame, n_row, n_col = features.shape
        n_lat = latent.shape[1]
        n_pos = n_row * n_col
        n_own = n_frame * n_pos
        n_halo = (4 * n_frame + 4) * SUB
        feat = jnp.transpose(features, (0, 2, 3, 4, 1)).reshape(n_own, n_chan)
        lat = jnp.transpose(latent, (0, 2, 3, 4, 1)).reshape(n_own, n_lat)
        wconv = jnp.transpose(conv_weight, (0, 1, 4, 5, 6, 2, 3)).reshape(4, 3, 9, n_chan, n_chan)
        wup = jnp.transpose(up_weight, (2, 3, 0, 1)).reshape(9, n_chan, n_chan)
        zyw = jnp.transpose(zy_weight, (0, 2, 1, 3))
        zbw = jnp.transpose(zb_weight, (0, 2, 1, 3))
        vmem = pl.BlockSpec(memory_space=pltpu.VMEM)
        hbm = pl.BlockSpec(memory_space=pl.ANY)
        wide = n_chan + LANES
        y = pl.pallas_call(
            functools.partial(kernel, n_sh, n_sw, (n_chan, n_frame, n_row, n_col, n_lat)),
            out_shape=jax.ShapeDtypeStruct((n_frame, 2 * n_row, 2 * n_col, n_chan), BF16),
            in_specs=[vmem] * 10 + [hbm] * 2,
            out_specs=vmem,
            scratch_shapes=[
                pltpu.VMEM((SLOTS, 3, n_chan, n_chan), BF16),
                pltpu.VMEM((3, n_frame, (n_row + 2) * SUB, n_chan), F32),
                pltpu.VMEM((n_own, n_chan), F32),
                pltpu.VMEM((n_own, n_chan), F32),
                pltpu.VMEM((n_halo, n_chan), F32),
                pltpu.VMEM((n_own + n_halo, n_chan), F32),
                pltpu.VMEM((n_own + n_halo, n_chan), F32),
                pltpu.VMEM((n_own + n_halo, LANES), F32),
                pltpu.VMEM((4, LANES, 2 * n_chan), BF16),
                pltpu.VMEM((4, SUB, n_chan), F32),
                pltpu.VMEM((n_chan, LANES), BF16),
                pltpu.VMEM((LANES, n_chan), BF16),
                pltpu.VMEM((2 * SUB, n_chan), F32),
                pltpu.VMEM((2, LANES), F32),
                pltpu.VMEM((2, n_dev, 2, LANES), F32),
                pltpu.VMEM((4, n_frame, SUB, wide), BF16),
                pltpu.VMEM((4, SUB, wide), BF16),
                pltpu.VMEM((2, 4, n_frame, SUB, wide), BF16),
                pltpu.VMEM((2, 4, SUB, wide), BF16),
                pltpu.VMEM((n_pos, n_chan), F32),
                pltpu.VMEM((2 * n_pos, n_chan), F32),
                pltpu.VMEM((n_own, n_chan), F32),
                pltpu.VMEM((3, 2, n_frame * (n_row + 1) * n_col, n_chan), F32),
                pltpu.VMEM((2, n_chan // LANES, 2 * n_col, LANES), F32),
                pltpu.SemaphoreType.DMA((SLOTS,)),
                pltpu.SemaphoreType.DMA,
                pltpu.SemaphoreType.DMA((2,)),
                pltpu.SemaphoreType.DMA((8,)),
                pltpu.SemaphoreType.DMA((2, 8)),
            ],
            compiler_params=pltpu.CompilerParams(collective_id=0, has_side_effects=True, vmem_limit_bytes=VMEM_BYTES),
        )(feat, lat, gn_gain, gn_bias, zy_bias, zb_bias, conv_bias, zyw, zbw, up_bias.reshape(1, n_chan), wconv, wup)
        return jnp.transpose(y.reshape(1, n_frame, 2 * n_row, 2 * n_col, n_chan), (0, 4, 1, 2, 3))

    data_spec = P("dp", None, None, "sh", "sw")
    return jax.shard_map(local_step, mesh=mesh, in_specs=(data_spec, data_spec) + (P(),) * 10, out_specs=data_spec, check_vma=False)
```

```python
import functools

import jax
import jax.numpy as jnp
from jax import lax
from jax.experimental import pallas as pl
from jax.experimental.pallas import tpu as pltpu
from jax.sharding import PartitionSpec as P

NUM_GROUPS = 32
GN_EPSILON = 1e-6
TILE = 256
LANES = 128
SUB = 8
SLOTS = 12
GROUP = 3
F32 = jnp.float32
BF16 = jnp.bfloat16
MESH = pl.DeviceIdType.MESH
VMEM_BYTES = 66 * 1000 * 1000
SIDES = ((0, (1, 0)), (1, (-1, 0)), (2, (0, 1)), (3, (0, -1)))
CORNERS = ((0, (1, 1)), (1, (1, -1)), (2, (-1, 1)), (3, (-1, -1)))


def split3(v):
    hi = v.astype(BF16)
    rest = v - hi.astype(F32)
    mid = rest.astype(BF16)
    low = (rest - mid.astype(F32)).astype(BF16)
    return hi, mid, low


def rounded(v):
    return v.astype(BF16).astype(F32)


def dot(a, b):
    return jnp.dot(a, b, preferred_element_type=F32)


def dot_nt(a, b):
    return lax.dot_general(a, b, (((1,), (1,)), ((), ())), preferred_element_type=F32)


def peer_steps(n_sh, n_sw):
    cores = 2 if n_sh % 2 == 0 else 1
    n_x = n_sh // cores
    steps = [(x, y, c) for x in range(n_x) for y in range(n_sw) for c in range(cores)][1:]
    return cores, n_x, sorted(steps, key=lambda s: -(min(s[0], n_x - s[0]) + min(s[1], n_sw - s[1])))


def kernel(n_sh, n_sw, dims, feat, lat, gain, shift, zyb, zbb, cb, zyw, zbw, upb, wconv, wup, out,
           ring, xs, rf, xf, hact, zy, zb, zf, zw, par, gm, gmt, sums, msg, peers, side_out, corner_out, side_in, corner_in,
           acc_0, acc_1, acc_2, tsum, yout, ring_sem, stat_send, stat_recv, halo_send, halo_recv):
    n_chan, n_frame, n_row, n_col, n_lat = dims
    n_pos = n_row * n_col
    n_own = n_frame * n_pos
    n_dev = n_sh * n_sw
    n_conv = 4
    n_tap = 9
    zlane = n_chan
    wide = n_chan + LANES
    sh = lax.axis_index("sh")
    sw = lax.axis_index("sw")
    me = sw * n_sh + sh
    per_group = n_chan // NUM_GROUPS
    count = float(per_group * n_own * n_dev)
    total = n_conv * n_tap + 3
    accs = (acc_0, acc_1, acc_2)

    def conv_copy(conv, tap, kt, slot):
        return pltpu.make_async_copy(wconv.at[conv, kt, tap], ring.at[slot, kt], ring_sem.at[slot])

    def up_copy(kh, kw, slot):
        return pltpu.make_async_copy(wup.at[kh * 3 + kw], ring.at[slot, kw], ring_sem.at[slot])

    def wait_chunk(slot):
        pltpu.make_async_copy(wconv.at[0, pl.ds(0, 3), 0], ring.at[slot], ring_sem.at[slot]).wait()

    def refill(g):
        nxt = g + SLOTS
        slot = lax.rem(g, SLOTS)

        @pl.when(nxt < n_conv * n_tap)
        def _():
            conv = nxt // n_tap
            for kt in range(3):
                conv_copy(conv, nxt - conv * n_tap, kt, slot).start()

        @pl.when((nxt >= n_conv * n_tap) & (nxt < total))
        def _():
            for kw in range(3):
                up_copy(nxt - n_conv * n_tap, kw, slot).start()

    cores, n_x, steps = peer_steps(n_sh, n_sw)
    chip = sh // cores
    core = sh - chip * cores

    def peer(step):
        return {"sh": lax.rem(chip + step[0], n_x) * cores + lax.rem(core + step[2], cores), "sw": lax.rem(sw + step[1], n_sw)}

    barrier = pltpu.get_barrier_semaphore()
    for step in steps:
        pl.semaphore_signal(barrier, inc=1, device_id=peer(step), device_id_type=MESH)
    for g in range(SLOTS):
        for kt in range(3):
            conv_copy(g // n_tap, g % n_tap, kt, g).start()

    def gather_rows(ref, at, step, n, cols):
        lanes = cols.stop - cols.start
        iota = lax.broadcasted_iota(jnp.int32, (SUB, lanes), 0)
        piece = jnp.zeros((SUB, lanes), F32)
        for i in range(n):
            row = jnp.broadcast_to(ref[at + i * step:at + i * step + 1, cols], (SUB, lanes))
            piece = jnp.where(iota == i, row, piece)
        return piece.astype(BF16)

    def stage(ref, lane0, lanes):
        cols = slice(0, lanes)
        put = slice(lane0, lane0 + lanes)
        for t in range(n_frame):
            base = t * n_pos
            side_out[0, t, :, put] = ref[base + n_pos - n_col:base + n_pos, cols].astype(BF16)
            side_out[1, t, :, put] = ref[base:base + n_col, cols].astype(BF16)
            side_out[2, t, :, put] = gather_rows(ref, base + n_col - 1, n_col, n_row, cols)
            side_out[3, t, :, put] = gather_rows(ref, base, n_col, n_row, cols)
        for d, at in enumerate((n_pos - 1, n_pos - n_col, n_col - 1, 0)):
            corner_out[d, :, put] = gather_rows(ref, at, n_pos, n_frame, cols)

    def inside(row, col):
        ok = None
        for step, pos, n in ((row, sh, n_sh), (col, sw, n_sw)):
            if step == 0:
                continue
            one = pos + step < n if step > 0 else pos + step >= 0
            ok = one if ok is None else ok & one
        return ok

    def halo_copies(slot):
        found = []
        for kind, (outs, ins, ways) in enumerate(((side_out, side_in, SIDES), (corner_out, corner_in, CORNERS))):
            for d, (row, col) in ways:
                copy = pltpu.make_async_remote_copy(
                    src_ref=outs.at[d], dst_ref=ins.at[slot, d], send_sem=halo_send.at[kind * 4 + d],
                    recv_sem=halo_recv.at[slot, kind * 4 + d], device_id={"sh": sh + row, "sw": sw + col}, device_id_type=MESH)
                found.append((copy, inside(row, col), inside(-row, -col)))
        return found

    def halo_start(slot):
        for copy, to, _ in halo_copies(slot):
            @pl.when(to)
            def _():
                copy.start()

    def halo_wait(slot):
        for copy, to, source in halo_copies(slot):
            @pl.when(source)
            def _():
                copy.wait_recv()

            @pl.when(to)
            def _():
                copy.wait_send()

    def stat_copy(slot, step):
        return pltpu.make_async_remote_copy(
            src_ref=msg, dst_ref=peers.at[slot, me], send_sem=stat_send, recv_sem=stat_recv.at[slot],
            device_id=peer(step), device_id_type=MESH)

    def stat_all(slot):
        part = peers.at[slot, pl.ds(0, n_dev - 1)]
        return pltpu.make_async_remote_copy(
            src_ref=part, dst_ref=part, send_sem=stat_send, recv_sem=stat_recv.at[slot], device_id=peer(steps[0]), device_id_type=MESH)

    def group_sums(slot, values):
        got = dot(jnp.concatenate(split3(values), axis=0), gm[...])
        rows = got[0:2 * SUB] + got[2 * SUB:4 * SUB] + got[4 * SUB:6 * SUB]
        mine = jnp.concatenate([jnp.sum(rows[0:SUB], axis=0, keepdims=True), jnp.sum(rows[SUB:], axis=0, keepdims=True)], axis=0)
        msg[...] = mine
        peers[slot, me] = mine

    def stats_send(slot):
        for step in steps:
            stat_copy(slot, step).start()

    def stats_finish(slot):
        both = stat_all(slot)
        both.wait_recv()
        both.wait_send()
        tot = jnp.sum(peers[slot], axis=0)
        mean = tot[0:1] / count
        var = jnp.maximum(tot[1:2] / count - jnp.square(mean), 0.0)
        inv = lax.rsqrt(var + GN_EPSILON)
        rows = lax.broadcasted_iota(jnp.int32, (SUB, LANES), 0)
        lhs = jnp.where(rows == 0, mean, jnp.where(rows == 1, inv, 0.0))
        got = dot(jnp.concatenate(split3(lhs), axis=0), gmt[...])
        whole = got[0:SUB] + got[SUB:2 * SUB] + got[2 * SUB:3 * SUB]
        return whole[0:1], whole[1:2]

    def latent_maps(conv):
        got = dot(zf[...].astype(BF16), zw[conv])
        zy[...] = got[:, 0:n_chan] + par[conv, 2:3, :]
        zb[...] = got[:, n_chan:] + par[conv, 3:4, :]

    halo_flags = [inside(-row, -col) for _, (row, col) in SIDES] + [inside(-row, -col) for _, (row, col) in CORNERS]

    def halo_values(slot, q):
        if q < 4 * n_frame:
            return side_in[slot, q // n_frame, q % n_frame, :, 0:n_chan].astype(F32), halo_flags[q // n_frame]
        return corner_in[slot, q - 4 * n_frame, :, 0:n_chan].astype(F32), halo_flags[4 + q - 4 * n_frame]

    n_side = n_frame * SUB
    sub_iota = lax.broadcasted_iota(jnp.int32, (SUB, n_chan), 0)

    def put_rows(t, at, mid, before, after):
        xs[1, t, pl.ds(at, SUB), :] = mid
        xs[0, t, pl.ds(at, SUB), :] = jnp.where(sub_iota == 0, before, pltpu.roll(mid, 1, axis=0))
        xs[2, t, pl.ds(at, SUB), :] = jnp.where(sub_iota == SUB - 1, after, pltpu.roll(mid, SUB - 1, axis=0))

    def build(slot, value_fn):
        for q in range(4 * n_frame + 4):
            v, flag = halo_values(slot, q)
            hact[q * SUB:(q + 1) * SUB, :] = jnp.where(flag, value_fn(v, n_own + q * SUB), 0.0)
        for t in range(n_frame):
            for at, side, corner in ((0, 0, 0), ((n_row + 1) * SUB, 1, 2)):
                mid = hact[side * n_side + t * SUB:side * n_side + (t + 1) * SUB, :]
                c0 = 4 * n_side + corner * SUB + t
                put_rows(t, at, mid, hact[c0:c0 + 1, :], hact[c0 + SUB:c0 + SUB + 1, :])

        def rows(g, carry):
            at = pl.multiple_of(g * SUB, SUB)
            t = g // n_row
            mid = value_fn(rf[pl.ds(at, SUB), :], at)
            put_rows(t, pl.multiple_of((g - t * n_row + 1) * SUB, SUB), mid, hact[pl.ds(2 * n_side + g, 1), :], hact[pl.ds(3 * n_side + g, 1), :])
            return carry

        lax.fori_loop(0, n_frame * n_row, rows, 0, unroll=4)

    for ref, g_dim, c_dim in ((gm, 1, 0), (gmt, 0, 1)):
        off = lax.broadcasted_iota(jnp.int32, ref.shape, c_dim) - lax.broadcasted_iota(jnp.int32, ref.shape, g_dim) * per_group
        ref[...] = jnp.where((off >= 0) & (off < per_group), 1.0, 0.0).astype(BF16)
    start = feat[...].astype(F32)
    rf[...] = start
    xf[...] = start
    group_sums(0, jnp.concatenate([jnp.sum(start.reshape(-1, SUB, n_chan), axis=0), jnp.sum(jnp.square(start).reshape(-1, SUB, n_chan), axis=0)], axis=0))
    pl.semaphore_wait(barrier, n_dev - 1)
    stats_send(0)
    zf[...] = jnp.zeros_like(zf)
    zf[0:n_own, 0:n_lat] = lat[...].astype(F32)
    stage(zf, zlane, LANES)
    stage(rf, 0, n_chan)
    halo_start(0)
    for b in range(2):
        for s in range(2):
            for row, ref in enumerate((gain, shift, zyb, zbb, cb)):
                par[2 * b + s, row:row + 1, :] = ref[b, s:s + 1, :]
    for which, ref in enumerate((zyw, zbw)):
        put = slice(which * n_chan, (which + 1) * n_chan)
        for b in range(2):
            rows_k = lax.broadcasted_iota(jnp.int32, (2 * SUB, n_chan), 0)
            w = [jnp.zeros((2 * SUB, n_chan), F32) for _ in range(2)]
            for k in range(n_lat):
                pair = ref[b, k].astype(F32)
                w = [jnp.where(rows_k == k, jnp.broadcast_to(pair[s:s + 1, :], rows_k.shape), w[s]) for s in range(2)]
            for s in range(2):
                zw[2 * b + s, 0:2 * SUB, put] = w[s].astype(BF16)
    zw[:, 2 * SUB:, :] = jnp.zeros((4, LANES - 2 * SUB, 2 * n_chan), BF16)

    def one_conv(conv, carry):
        slot = lax.rem(conv, 2)
        halo_wait(slot)

        @pl.when(conv == 0)
        def _():
            for q in range(4 * n_frame):
                zf[n_own + q * SUB:n_own + (q + 1) * SUB, :] = side_in[slot, q // n_frame, q % n_frame, :, zlane:wide].astype(F32)
            for q in range(4):
                at = n_own + (4 * n_frame + q) * SUB
                zf[at:at + SUB, :] = corner_in[slot, q, :, zlane:wide].astype(F32)

        latent_maps(conv)
        for ref in accs:
            ref[...] = jnp.zeros_like(ref)
        mean, inv = stats_finish(slot)
        scale = inv * par[conv, 0:1, :]
        offset = par[conv, 1:2, :]

        def act(v, at):
            normed = (v - mean) * scale + offset
            mixed = normed * zy[pl.ds(at, SUB), :] + zb[pl.ds(at, SUB), :]
            return rounded(mixed / (1.0 + jnp.exp(-mixed)))

        build(slot, act)

        def taps(step, carry):
            for i in range(GROUP):
                wait_chunk(lax.rem(conv * n_tap + step * GROUP + i, SLOTS))
            for kt in (2, 1, 0):
                lhs, rhs = [], []
                for i in range(GROUP):
                    p = step * GROUP + i
                    kh = p // 3
                    kw = p - 3 * kh
                    at = pl.multiple_of(kh * SUB, SUB)
                    lhs.append(xs[kw, 0:kt + 1, pl.ds(at, n_pos), :].reshape((kt + 1) * n_pos, n_chan).astype(BF16))
                    rhs.append(ring[lax.rem(conv * n_tap + p, SLOTS), kt])
                accs[kt][...] += dot_nt(jnp.concatenate(lhs, axis=1), jnp.concatenate(rhs, axis=1))
            @pl.when(step < n_tap // GROUP - 1)
            def _():
                for i in range(GROUP):
                    refill(conv * n_tap + step * GROUP + i)
            return carry

        lax.fori_loop(0, n_tap // GROUP, taps, 0)

        odd = lax.rem(conv, 2) == 1
        s1 = jnp.zeros((SUB, n_chan), F32)
        s2 = jnp.zeros((SUB, n_chan), F32)
        bias = par[conv, 4:5, :]
        for at in range(0, n_pos, SUB):
            shared = acc_0[at:at + SUB, :] + bias
            for t in range(n_frame):
                early = max(t - 1, 0) * n_pos + at
                row = t * n_pos + at
                y = rounded(acc_2[row:row + SUB, :] + acc_1[early:early + SUB, :] + shared)
                old = xf[row:row + SUB, :]
                x = jnp.where(odd, rounded(old + y), y)
                xf[row:row + SUB, :] = jnp.where(odd, x, old)
                rf[row:row + SUB, :] = x
                s1 += x
                s2 += jnp.square(x)
        after = 1 - slot
        group_sums(after, jnp.concatenate([s1, s2], axis=0))

        @pl.when(conv < n_conv - 1)
        def _():
            stats_send(after)

        stage(rf, 0, n_chan)
        halo_start(after)
        for i in range(n_tap - GROUP, n_tap):
            refill(conv * n_tap + i)
        return carry

    lax.fori_loop(0, n_conv, one_conv, 0)

    last = n_conv % 2
    halo_wait(last)
    build(last, lambda v, at: v)
    n_up = (n_row + 1) * n_col
    m_up = n_frame * n_up

    def up_row(kh, carry):
        ring_slot = lax.rem(n_conv * n_tap + kh, SLOTS)
        wait_chunk(ring_slot)
        at = pl.multiple_of(jnp.minimum(kh, 1) * SUB, SUB)
        x = [xs[d, :, pl.ds(at, n_up), :].reshape(m_up, n_chan).astype(BF16) for d in range(3)]
        for n in range(n_chan // TILE):
            cols = slice(n * TILE, (n + 1) * TILE)
            side_a = dot_nt(jnp.concatenate([x[0], x[1]], axis=0), ring[ring_slot, 0, cols, :])
            both = dot_nt(x[1], ring[ring_slot, 1, cols, :])
            side_b = dot_nt(jnp.concatenate([x[1], x[2]], axis=0), ring[ring_slot, 2, cols, :])
            tsum[kh, 0, :, cols] = side_a[0:m_up] + both + side_b[0:m_up]
            tsum[kh, 1, :, cols] = side_a[m_up:] + both + side_b[m_up:]
        return carry

    lax.fori_loop(0, 3, up_row, 0)
    bias_up = upb[...]

    def finish(g, carry):
        t = g // n_row
        i = g - t * n_row
        here = t * n_up + i * SUB
        for a in range(2):
            for b in range(2):
                v = bias_up
                for kh in range(3):
                    down = SUB if (a == 1 and kh != 1) else 0
                    v = v + tsum[kh, b, pl.ds(pl.multiple_of(here + down, SUB), SUB), :]
                for j in range(n_chan // LANES):
                    yout[a, j, pl.ds(b, SUB, stride=2), :] = v[:, j * LANES:(j + 1) * LANES]
            for j in range(n_chan // LANES):
                out[t, 2 * i + a, :, j * LANES:(j + 1) * LANES] = yout[a, j].astype(BF16)
        return carry

    lax.fori_loop(0, n_frame * n_row, finish, 0)


def solution(mesh):
    n_sh = mesh.shape["sh"]
    n_sw = mesh.shape["sw"]
    n_dev = n_sh * n_sw

    def local_step(features, latent, gn_gain, gn_bias, zy_weight, zy_bias, zb_weight, zb_bias, conv_weight, conv_bias, up_weight, up_bias):
        _, n_chan, n_frame, n_row, n_col = features.shape
        n_lat = latent.shape[1]
        n_pos = n_row * n_col
        n_own = n_frame * n_pos
        n_halo = (4 * n_frame + 4) * SUB
        feat = jnp.transpose(features, (0, 2, 3, 4, 1)).reshape(n_own, n_chan)
        lat = jnp.transpose(latent, (0, 2, 3, 4, 1)).reshape(n_own, n_lat)
        wconv = jnp.transpose(conv_weight, (0, 1, 4, 5, 6, 2, 3)).reshape(4, 3, 9, n_chan, n_chan)
        wup = jnp.transpose(up_weight, (2, 3, 0, 1)).reshape(9, n_chan, n_chan)
        zyw = jnp.transpose(zy_weight, (0, 2, 1, 3))
        zbw = jnp.transpose(zb_weight, (0, 2, 1, 3))
        vmem = pl.BlockSpec(memory_space=pltpu.VMEM)
        hbm = pl.BlockSpec(memory_space=pl.ANY)
        wide = n_chan + LANES
        y = pl.pallas_call(
            functools.partial(kernel, n_sh, n_sw, (n_chan, n_frame, n_row, n_col, n_lat)),
            out_shape=jax.ShapeDtypeStruct((n_frame, 2 * n_row, 2 * n_col, n_chan), BF16),
            in_specs=[vmem] * 10 + [hbm] * 2,
            out_specs=vmem,
            scratch_shapes=[
                pltpu.VMEM((SLOTS, 3, n_chan, n_chan), BF16),
                pltpu.VMEM((3, n_frame, (n_row + 2) * SUB, n_chan), F32),
                pltpu.VMEM((n_own, n_chan), F32),
                pltpu.VMEM((n_own, n_chan), F32),
                pltpu.VMEM((n_halo, n_chan), F32),
                pltpu.VMEM((n_own + n_halo, n_chan), F32),
                pltpu.VMEM((n_own + n_halo, n_chan), F32),
                pltpu.VMEM((n_own + n_halo, LANES), F32),
                pltpu.VMEM((4, LANES, 2 * n_chan), BF16),
                pltpu.VMEM((4, SUB, n_chan), F32),
                pltpu.VMEM((n_chan, LANES), BF16),
                pltpu.VMEM((LANES, n_chan), BF16),
                pltpu.VMEM((2 * SUB, n_chan), F32),
                pltpu.VMEM((2, LANES), F32),
                pltpu.VMEM((2, n_dev, 2, LANES), F32),
                pltpu.VMEM((4, n_frame, SUB, wide), BF16),
                pltpu.VMEM((4, SUB, wide), BF16),
                pltpu.VMEM((2, 4, n_frame, SUB, wide), BF16),
                pltpu.VMEM((2, 4, SUB, wide), BF16),
                pltpu.VMEM((n_pos, n_chan), F32),
                pltpu.VMEM((2 * n_pos, n_chan), F32),
                pltpu.VMEM((n_own, n_chan), F32),
                pltpu.VMEM((3, 2, n_frame * (n_row + 1) * n_col, n_chan), F32),
                pltpu.VMEM((2, n_chan // LANES, 2 * n_col, LANES), F32),
                pltpu.SemaphoreType.DMA((SLOTS,)),
                pltpu.SemaphoreType.DMA,
                pltpu.SemaphoreType.DMA((2,)),
                pltpu.SemaphoreType.DMA((8,)),
                pltpu.SemaphoreType.DMA((2, 8)),
            ],
            compiler_params=pltpu.CompilerParams(collective_id=0, has_side_effects=True, vmem_limit_bytes=VMEM_BYTES),
        )(feat, lat, gn_gain, gn_bias, zy_bias, zb_bias, conv_bias, zyw, zbw, up_bias.reshape(1, n_chan), wconv, wup)
        return jnp.transpose(y.reshape(1, n_frame, 2 * n_row, 2 * n_col, n_chan), (0, 4, 1, 2, 3))

    data_spec = P("dp", None, None, "sh", "sw")
    return jax.shard_map(local_step, mesh=mesh, in_specs=(data_spec, data_spec) + (P(),) * 10, out_specs=data_spec, check_vma=False)
```
